512 devices in a mesh: site: 2 (over core), rows: 8 (over z), cols: 32 (over y, x).
Axes of the slice: x: 4, y: 8, z: 8, core: 2. Of those that a mesh axis runs over, the one named last changes fastest.
Arguments:
- tracer: float32 [512, 1024, 128], P(('site', 'rows'), 'cols'), parts along dimension 0, may hold values from 0.5 to 2
- flow_y: float32 [512, 1024, 128], P(('site', 'rows'), 'cols'), parts along dimension 0, may hold values from -0.3 to 0.3
- flow_x: float32 [512, 1024, 128], P(('site', 'rows'), 'cols'), parts along dimension 0, may hold values from -0.3 to 0.3
Outputs:
- scaled_field: float32 [512, 1024, 128], P(('site', 'rows'), 'cols'), parts along dimension 0
- tracer_end: float32 [512, 1024, 128], P(('site', 'rows'), 'cols'), parts along dimension 0
The draws below stay inside these ranges and needn't reach their ends.
There are 2 independent parts, one for each index of `site`. The reference program is written for one: setup_inputs(seed, part) draws one part's arguments, and reference() takes and returns one part's arrays. A program takes and returns all parts, laid end to end along the dimension named above; each array names one. Nothing has to cross between parts.
All inputs are finite; a program needn't handle non-finite values.
Results may differ from the reference program's by a relative error of at most 0.00002.
Values sent between devices are 32-bit elements; how exact they have to be, the bound alone decides.
No kernel may reach another device: no remote copies, remote signals or barrier semaphores. Data moves between devices by JAX's collectives and lax.ppermute only.
A program may use at most 64 MiB of HBM per device.

```python
import jax
import jax.numpy as jnp
from jax import lax

GRID_Y = 256
GRID_X = 1024
SPECIES = 128
STEPS = 6


def block_levels(rng, shape, cuts, low, top_value):
    def one(dim, parts):
        heights = jax.random.uniform(jax.random.fold_in(jax.random.fold_in(rng, 6), dim), (parts,), jnp.float32, low / len(cuts), top_value / len(cuts))
        return jnp.repeat(jnp.exp(heights), shape[dim] // parts).reshape((-1,) + (1,) * (len(shape) - dim - 1))

    factor_of = one(*cuts[0])
    for cut in cuts[1:]:
        factor_of = factor_of * one(*cut)
    return factor_of


def setup_inputs(seed: int = 0, part: int = 0) -> dict:
    streams_of = jax.random.split(jax.random.key(seed), 4)
    part_splits = jax.random.split(jax.random.fold_in(streams_of[3], part), 4)
    return {
        "tracer": jnp.clip(0.5 + 1.5 * jax.random.uniform(part_splits[0], (GRID_Y, GRID_X, SPECIES), jnp.float32) ** block_levels(part_splits[0], (GRID_Y, GRID_X, SPECIES), ((0, 8), (1, 32)), -0.2, 0.2), 0.5, 2.0),
        "flow_y": jnp.clip(jax.random.uniform(part_splits[1], (GRID_Y, GRID_X, SPECIES), jnp.float32, -0.3, 0.3) * block_levels(part_splits[1], (GRID_Y, GRID_X, SPECIES), ((0, 8), (1, 32)), -0.4, 0.0), -0.3, 0.3),
        "flow_x": jnp.clip(jax.random.uniform(part_splits[2], (GRID_Y, GRID_X, SPECIES), jnp.float32, -0.3, 0.3) * block_levels(part_splits[2], (GRID_Y, GRID_X, SPECIES), ((0, 8), (1, 32)), -0.4, 0.0), -0.3, 0.3),
    }


def strip_edges(values, dims):
    for dim in dims:
        values = lax.slice_in_dim(values, 1, values.shape[dim] - 1, axis=dim)
    return values

def neighbour(values, dim, start, dims):
    others = [other for other in dims if other != dim]
    values = strip_edges(values, others)
    return lax.slice_in_dim(values, start, start + values.shape[dim] - 2, axis=dim)

def one_step(padded, flow_y, flow_x):
    middle = strip_edges(padded, (0, 1))
    lower = [neighbour(padded, dim, 0, (0, 1)) for dim in (0, 1)]
    upper = [neighbour(padded, dim, 2, (0, 1)) for dim in (0, 1)]
    slopes = [above - below for above, below in zip(upper, lower)]
    smooth_rate = 0.05
    spread = lower[0] + upper[0] + lower[1] + upper[1] - 4.0 * middle
    return middle - flow_y * slopes[0] - flow_x * slopes[1] + smooth_rate * spread

def reference(tracer, flow_y, flow_x):
    for step in range(STEPS):
        tracer = one_step(jnp.pad(tracer, ((1, 1), (1, 1), (0, 0)), mode='constant'), flow_y, flow_x)
    line_mean = lax.optimization_barrier(jnp.mean(tracer, axis=1, keepdims=True))
    centred = tracer - line_mean
    line_variance = lax.optimization_barrier(jnp.mean(centred * centred, axis=1, keepdims=True))
    scaled_field = centred * lax.rsqrt(line_variance + 0.0001)
    return (scaled_field, tracer)
```

```python
import jax
import jax.numpy as jnp
from jax import lax
from jax.sharding import Mesh, PartitionSpec as P

STEPS = 6
COLS = ("y", "x")


def neighbours(block, axis, dim, low, high):
    count = lax.axis_size(axis) if isinstance(axis, str) else 32
    forward = [(i, i + 1) for i in range(count - 1)]
    backward = [(target, source) for source, target in forward]
    return lax.ppermute(high, axis, forward), lax.ppermute(low, axis, backward)


def sum_over(values, axis):
    count = lax.axis_size(axis)
    copies = jnp.broadcast_to(values, (count, *values.shape))
    return jnp.sum(lax.all_to_all(copies, axis, 0, 0, tiled=True), axis=0)


def strip_edges(values, dims):
    for dim in dims:
        values = lax.slice_in_dim(values, 1, values.shape[dim] - 1, axis=dim)
    return values


def neighbour(values, dim, start, dims):
    others = [other for other in dims if other != dim]
    values = strip_edges(values, others)
    return lax.slice_in_dim(values, start, start + values.shape[dim] - 2, axis=dim)


def one_step(padded, flow_y, flow_x):
    middle = strip_edges(padded, (0, 1))
    lower = [neighbour(padded, dim, 0, (0, 1)) for dim in (0, 1)]
    upper = [neighbour(padded, dim, 2, (0, 1)) for dim in (0, 1)]
    slopes = [above - below for above, below in zip(upper, lower)]
    smooth_rate = 0.05
    spread = lower[0] + upper[0] + lower[1] + upper[1] - 4.0 * middle
    return middle - flow_y * slopes[0] - flow_x * slopes[1] + smooth_rate * spread


def shards(tracer, flow_y, flow_x):
    size = tracer.shape[0]
    width, inner = STEPS, STEPS - 1
    parts = (tracer, flow_y, flow_x)
    widths = (width, inner, inner)
    low = jnp.concatenate([p[:w] for p, w in zip(parts, widths)], axis=0)
    high = jnp.concatenate([p[size - w :] for p, w in zip(parts, widths)], axis=0)
    before, after = neighbours(None, "rows", 0, low, high)
    cuts = ((0, width), (width, width + inner), (width + inner, width + 2 * inner))
    parts = [
        jnp.concatenate([before[b:e], p, after[b:e]], axis=0) for p, (b, e) in zip(parts, cuts)
    ]
    tall = [parts[0]] + [jnp.pad(p, ((1, 1), (0, 0), (0, 0))) for p in parts[1:]]
    low = jnp.concatenate([p[:, :w] for p, w in zip(tall, widths)], axis=1)
    high = jnp.concatenate([p[:, size - w :] for p, w in zip(tall, widths)], axis=1)
    before, after = neighbours(None, COLS, 1, low, high)
    padded = jnp.concatenate([before[:, :width], parts[0], after[:, :width]], axis=1)
    wide_flow_y, wide_flow_x = [
        jnp.concatenate([before[1:-1, b:e], p, after[1:-1, b:e]], axis=1)
        for p, (b, e) in zip(parts[1:], cuts[1:])
    ]
    for step in range(STEPS):
        values = one_step(padded, wide_flow_y, wide_flow_x)
        margin = STEPS - 1 - step
        place = lax.axis_index("rows") * tracer.shape[0] - margin + jnp.arange(values.shape[0])
        keep_cells = (place >= 0) & (place < tracer.shape[0] * lax.axis_size("rows"))
        values = jnp.where(keep_cells.reshape((-1,) + (1,) * 2), values, 0.0)
        place = lax.axis_index(COLS) * tracer.shape[1] - margin + jnp.arange(values.shape[1])
        keep_cells = (place >= 0) & (place < tracer.shape[1] * 32)
        values = jnp.where(keep_cells.reshape((-1,) + (1,) * 1), values, 0.0)
        if step < STEPS - 1:
            wide_flow_y = strip_edges(wide_flow_y, (0, 1))
            wide_flow_x = strip_edges(wide_flow_x, (0, 1))
        padded = values
    tracer = padded
    count = tracer.shape[1] * 32
    guess = 1.0
    moved = tracer - guess
    both = jnp.concatenate([jnp.sum(moved, axis=1), jnp.sum(moved * moved, axis=1)], axis=0)
    both = sum_over(sum_over(both, "x"), "y")
    totals, squares = both[:size, None], both[size:, None]
    line_mean = guess + totals / count
    centred = tracer - line_mean
    line_variance = squares / count - totals / count * (totals / count)
    scaled_field = centred * lax.rsqrt(line_variance + 0.0001)
    return (scaled_field, tracer)


def solution(mesh):
    mesh = Mesh(mesh.devices.reshape(2, 8, 8, 4), ("site", "rows", "y", "x"))
    placed = P(("site", "rows"), COLS, None)
    return jax.shard_map(
        shards, mesh=mesh, in_specs=(placed,) * 3, out_specs=(placed,) * 2, check_vma=False
    )
```

```python
import jax
import jax.numpy as jnp
from jax import lax
from jax.sharding import Mesh, PartitionSpec as P

STEPS = 6
ROWS = "rows"
COLS = ("y", "x")
COUNT = {ROWS: 8, COLS: 32}


def swap_with(block, axis, odd):
    pairs = []
    for low in range(odd, COUNT[axis] - 1, 2):
        pairs += [(low, low + 1), (low + 1, low)]
    return lax.ppermute(block, axis, pairs)


def sum_over(values, axis):
    count = lax.axis_size(axis)
    copies = jnp.broadcast_to(values, (count, *values.shape))
    return jnp.sum(lax.all_to_all(copies, axis, 0, 0, tiled=True), axis=0)


def edge(values, dim, width, top):
    size = values.shape[dim]
    return lax.dynamic_slice_in_dim(values, jnp.where(top, size - width, 0), width, axis=dim)


def edges(parts, dim, widths, top):
    return jnp.concatenate([edge(p, dim, w, top) for p, w in zip(parts, widths)], axis=dim)


def strip_edges(values, dims):
    for dim in dims:
        values = lax.slice_in_dim(values, 1, values.shape[dim] - 1, axis=dim)
    return values


def neighbour(values, dim, start, dims):
    others = [other for other in dims if other != dim]
    values = strip_edges(values, others)
    return lax.slice_in_dim(values, start, start + values.shape[dim] - 2, axis=dim)


def one_step(padded, flow_y, flow_x):
    middle = strip_edges(padded, (0, 1))
    lower = [neighbour(padded, dim, 0, (0, 1)) for dim in (0, 1)]
    upper = [neighbour(padded, dim, 2, (0, 1)) for dim in (0, 1)]
    slopes = [above - below for above, below in zip(upper, lower)]
    smooth_rate = 0.05
    spread = lower[0] + upper[0] + lower[1] + upper[1] - 4.0 * middle
    return middle - flow_y * slopes[0] - flow_x * slopes[1] + smooth_rate * spread


def shards(tracer, flow_y, flow_x):
    size = tracer.shape[0]
    width, inner = STEPS, STEPS - 1
    parts = (tracer, flow_y, flow_x)
    widths = (width, inner, inner)
    cuts = ((0, width), (width, width + inner), (width + inner, width + 2 * inner))
    even_row = lax.axis_index(ROWS) % 2 == 0
    even_col = lax.axis_index(COLS) % 2 == 0

    row_b = swap_with(edges(parts, 0, widths, ~even_row), ROWS, 1)
    row_a = swap_with(edges(parts, 0, widths, even_row), ROWS, 0)
    col_b = swap_with(edges(parts, 1, widths, ~even_col), COLS, 1)
    col_a = swap_with(edges(parts, 1, widths, even_col), COLS, 0)
    south, north = jnp.where(even_row, row_b, row_a), jnp.where(even_row, row_a, row_b)
    west, east = jnp.where(even_col, col_b, col_a), jnp.where(even_col, col_a, col_b)

    south, north = [[v[b:e] for b, e in cuts] for v in (south, north)]
    far, near = width - 1, inner - 1

    def corner(top):
        rows = []
        for (t, fy, fx), last in ((south, True), (north, False)):
            pick = lambda v, n: v[v.shape[0] - n :] if last else v[:n]
            flows = jnp.concatenate([edge(pick(f, near), 1, near, top) for f in (fy, fx)], axis=1)
            cells = edge(pick(t, far), 1, far, top)
            rows += [jnp.pad(cells, ((0, 0), (0, 2 * near - far), (0, 0))), flows]
        return jnp.concatenate(rows, axis=0)

    cor_b = swap_with(corner(~even_col), COLS, 1)
    cor_a = swap_with(corner(even_col), COLS, 0)
    cor_w, cor_e = jnp.where(even_col, cor_b, cor_a), jnp.where(even_col, cor_a, cor_b)

    def side(main, cor, k, is_west):
        b, e = cuts[k]
        middle = main[:, b:e]
        if k == 0:
            low, high = cor[0:far, :far], cor[far + near : far + near + far, :far]
        else:
            c = slice((k - 1) * near, k * near)
            low, high = cor[far : far + near, c], cor[2 * far + near :, c]
        sides = ((0, 0), (1, 0) if is_west else (0, 1), (0, 0))
        low = jnp.pad(jnp.pad(low, sides), ((1, 0), (0, 0), (0, 0)))
        high = jnp.pad(jnp.pad(high, sides), ((0, 1), (0, 0), (0, 0)))
        return jnp.concatenate([low, middle, high], axis=0)

    whole = []
    for k in range(3):
        tall = jnp.concatenate([south[k], parts[k], north[k]], axis=0)
        whole.append(
            jnp.concatenate([side(west, cor_w, k, True), tall, side(east, cor_e, k, False)], axis=1)
        )
    padded, wide_flow_y, wide_flow_x = whole
    for step in range(STEPS):
        values = one_step(padded, wide_flow_y, wide_flow_x)
        margin = STEPS - 1 - step
        place = lax.axis_index(ROWS) * size - margin + jnp.arange(values.shape[0])
        keep_cells = (place >= 0) & (place < size * COUNT[ROWS])
        values = jnp.where(keep_cells.reshape((-1,) + (1,) * 2), values, 0.0)
        place = lax.axis_index(COLS) * size - margin + jnp.arange(values.shape[1])
        keep_cells = (place >= 0) & (place < size * COUNT[COLS])
        values = jnp.where(keep_cells.reshape((-1,) + (1,) * 1), values, 0.0)
        if step < STEPS - 1:
            wide_flow_y = strip_edges(wide_flow_y, (0, 1))
            wide_flow_x = strip_edges(wide_flow_x, (0, 1))
        padded = values
    tracer = padded
    count = size * COUNT[COLS]
    guess = 1.0
    moved = tracer - guess
    both = jnp.concatenate([jnp.sum(moved, axis=1), jnp.sum(moved * moved, axis=1)], axis=0)
    both = sum_over(sum_over(both, "x"), "y")
    totals, squares = both[:size, None], both[size:, None]
    line_mean = guess + totals / count
    centred = tracer - line_mean
    line_variance = squares / count - totals / count * (totals / count)
    scaled_field = centred * lax.rsqrt(line_variance + 0.0001)
    return (scaled_field, tracer)


def solution(mesh):
    mesh = Mesh(mesh.devices.reshape(2, 8, 8, 4), ("site", "rows", "y", "x"))
    placed = P(("site", "rows"), COLS, None)
    return jax.shard_map(
        shards, mesh=mesh, in_specs=(placed,) * 3, out_specs=(placed,) * 2, check_vma=False
    )
```

```python
import functools

import jax
import jax.numpy as jnp
from jax import lax
from jax.experimental import pallas as pl
from jax.experimental.pallas import tpu as pltpu
from jax.sharding import Mesh, PartitionSpec as P

STEPS = 6
SIZE = 32
LANES = 128
ROWS = "rows"
COLS = ("y", "x")
HALO = STEPS
TALL = SIZE + 2 * HALO
WIDE = SIZE + 16
BLOCK = slice(HALO, HALO + SIZE)
CENTRE = slice(8, 8 + SIZE)
WORK = (TALL, WIDE, LANES)
GUESS = 1.0
F32 = jnp.float32
VMEM = pl.BlockSpec(memory_space=pltpu.VMEM)


def size_of(axis):
    sizes = [lax.axis_size(a) for a in ((axis,) if isinstance(axis, str) else axis)]
    return functools.reduce(lambda a, b: a * b, sizes)


def swap_with(block, axis, odd):
    pairs = []
    for low in range(odd, size_of(axis) - 1, 2):
        pairs += [(low, low + 1), (low + 1, low)]
    return lax.ppermute(block, axis, pairs)


def turned(tiles, shift):
    return pltpu.roll(tiles, shift % 8, axis=tiles.ndim - 2)


def pack_kernel(t_in, fy_in, fx_in, t, fy, fx, col_a, col_b, row_a, row_b, sems):
    blocks = ((t_in, t), (fy_in, fy), (fx_in, fx))
    copies = [pltpu.make_async_copy(src, dst, sems.at[k]) for k, (src, dst) in enumerate(blocks)]
    for copy in copies:
        copy.start()
    even_row = lax.axis_index(ROWS) % 2 == 0
    even_col = lax.axis_index(COLS) % 2 == 0
    sub = lax.broadcasted_iota(jnp.int32, (SIZE, 8, LANES), 1)
    for copy in copies:
        copy.wait()
    t_low, fy_low, fx_low = [v[:, 0:8] for v in (t, fy, fx)]
    t_high, fy_high, fx_high = [v[:, SIZE - 8 :] for v in (t, fy, fx)]
    first = (
        jnp.where(sub < 6, t_low, turned(fx_low, 6)),
        jnp.where(sub < 5, fy_low, turned(fx_low, 3)),
    )
    last = (
        jnp.where(sub >= 2, t_high, turned(fx_high, 5)),
        jnp.where(sub >= 3, fy_high, turned(fx_high, 3)),
    )
    for k in range(2):
        col_a[:, 8 * k : 8 * k + 8] = jnp.where(even_col, last[k], first[k])
        col_b[:, 8 * k : 8 * k + 8] = jnp.where(even_col, first[k], last[k])
    for out, top in ((row_a, even_row), (row_b, jnp.logical_not(even_row))):
        out[0:6] = t[pl.ds(jnp.where(top, SIZE - 6, 0), 6)]
        out[6:11] = fy[pl.ds(jnp.where(top, SIZE - 5, 0), 5)]
        out[11:16] = fx[pl.ds(jnp.where(top, SIZE - 5, 0), 5)]


def corner_kernel(col_a, col_b, cor_a, cor_b):
    even_row = lax.axis_index(ROWS) % 2 == 0
    for out, top in ((cor_a, even_row), (cor_b, jnp.logical_not(even_row))):
        at = pl.ds(jnp.where(top, SIZE - STEPS + 1, 0), STEPS - 1)
        out[:, 0:16] = col_a[at]
        out[:, 16:32] = col_b[at]


def sum_kernel(parts, out):
    total = jnp.sum(parts[...], axis=0)
    for k in range(out.shape[0]):
        out[k] = total


def beside(packed, west):
    one, two = packed[:, 0:8], packed[:, 8:16]
    sub = lax.broadcasted_iota(jnp.int32, one.shape, 1)
    if west:
        return one, two, jnp.where(sub < 5, turned(one, 3), turned(two, 5))
    return one, two, jnp.where(sub < 2, turned(one, 2), turned(two, 5))


def steps_kernel(t, fy, fx, col_a, col_b, row_a, row_b, cor_a, cor_b, end, sums, p0, p1, cy, cx):
    for src, dst in ((t, p0), (fy, cy), (fx, cx)):
        dst[BLOCK, CENTRE] = src[...]
    row, col = lax.axis_index(ROWS), lax.axis_index(COLS)
    even_row, even_col = row % 2 == 0, col % 2 == 0
    first_row, last_row = row == 0, row == lax.axis_size(ROWS) - 1
    has_west, has_east = col > 0, col < size_of(COLS) - 1
    west, east = jnp.where(even_col, col_b[...], col_a[...]), jnp.where(even_col, col_a[...], col_b[...])
    south, north = jnp.where(even_row, row_b[...], row_a[...]), jnp.where(even_row, row_a[...], row_b[...])
    cuts = ((0, 6), (6, 11), (11, 16))
    for v, at, is_west in ((west, 0, True), (east, 8 + SIZE, False)):
        for tile, dst in zip(beside(v, is_west), (p0, cy, cx)):
            dst[BLOCK, at : at + 8] = tile
    for (b, e), dst in zip(cuts, (p0, cy, cx)):
        dst[HALO - (e - b) : HALO, CENTRE] = south[b:e]
        dst[HALO + SIZE : HALO + SIZE + e - b, CENTRE] = north[b:e]
    south, north = jnp.where(even_row, cor_b[...], cor_a[...]), jnp.where(even_row, cor_a[...], cor_b[...])
    for v, rows in ((south, slice(1, HALO)), (north, slice(HALO + SIZE, TALL - 1))):
        of_a, of_b = v[:, 0:16], v[:, 16:32]
        for packed, at, is_west in (
            (jnp.where(even_col, of_b, of_a), 0, True),
            (jnp.where(even_col, of_a, of_b), 8 + SIZE, False),
        ):
            for tile, dst in zip(beside(packed, is_west), (p0, cy, cx)):
                dst[rows, at : at + 8] = tile

    @pl.when(first_row)
    def _():
        p1[0:HALO] = jnp.zeros((HALO, WIDE, LANES), F32)

    @pl.when(last_row)
    def _():
        p1[HALO + SIZE :] = jnp.zeros((HALO, WIDE, LANES), F32)

    sub = lax.broadcasted_iota(jnp.int32, (8, LANES), 0)
    lowest, highest = sub == 0, sub == 7
    low_rows, high_rows = jnp.where(first_row, HALO, 0), jnp.where(last_row, HALO + SIZE, TALL)

    def stepped(src, y, tiles):
        j0, j1 = tiles[0], tiles[-1] + 1
        around = range(max(j0 - 1, 0), min(j1 + 1, WIDE // 8))
        at = lambda j: pl.ds(8 * j, 8)
        mid = {j: src[y, at(j)] for j in around}
        up = {j: turned(v, 1) for j, v in mid.items()}
        down = {j: turned(v, -1) for j, v in mid.items()}
        out = []
        for j in tiles:
            below, above = src[y - 1, at(j)], src[y + 1, at(j)]
            left = jnp.where(lowest, up[j - 1], up[j]) if j - 1 in up else up[j]
            right = jnp.where(highest, down[j + 1], down[j]) if j + 1 in down else down[j]
            spread = below + above + left + right - 4.0 * mid[j]
            new = mid[j] - cy[y, at(j)] * (above - below) - cx[y, at(j)] * (right - left) + 0.05 * spread
            if j == 0:
                new = jnp.where(has_west, new, 0.0)
            if j == WIDE // 8 - 1:
                new = jnp.where(has_east, new, 0.0)
            out.append(new)
        return out

    src, dst = p0, p1
    for step in range(1, STEPS):
        tiles = list(range(WIDE // 8))

        def body(y, _, src=src, dst=dst):
            for j, new in zip(tiles, stepped(src, y, tiles)):
                dst[y, pl.ds(8 * j, 8)] = new
            return 0

        lax.fori_loop(jnp.maximum(step, low_rows), jnp.minimum(TALL - step, high_rows), body, 0)
        src, dst = dst, src

    tiles = list(range(1, 1 + SIZE // 8))

    def final(y, _):
        new = stepped(src, y + HALO, tiles)
        moved = [v - GUESS for v in new]
        for j, v in enumerate(new):
            end[y, pl.ds(8 * j, 8)] = v
        total, square = moved[0], moved[0] * moved[0]
        for v in moved[1:]:
            total, square = total + v, square + v * v
        cy[y, 0:8] = total
        cx[y, 0:8] = square
        return 0

    lax.fori_loop(0, SIZE, final, 0)
    total = jnp.sum(cy[0:SIZE, 0:8], axis=1)
    square = jnp.sum(cx[0:SIZE, 0:8], axis=1)
    for k in range(sums.shape[0]):
        sums[k, 0:SIZE] = total
        sums[k, SIZE : 2 * SIZE] = square


def call(kernel, args, outs, scratch, in_specs=None):
    specs = in_specs or [VMEM] * len(args)
    return pl.pallas_call(
        kernel,
        out_shape=[pltpu.VMEM(shape, F32) for shape in outs],
        in_specs=specs,
        out_specs=[VMEM] * len(outs),
        scratch_shapes=scratch,
        compiler_params=pltpu.CompilerParams(vmem_limit_bytes=16 * 2**20),
    )(*[pltpu.with_memory_space_constraint(a, s.memory_space) for a, s in zip(args, specs)])


def shards(tracer, flow_y, flow_x):
    columns, rows = (SIZE, 16, LANES), (16, SIZE, LANES)
    *blocks, col_a, col_b, row_a, row_b = call(
        pack_kernel,
        (tracer, flow_y, flow_x),
        (tracer.shape,) * 3 + (columns,) * 2 + (rows,) * 2,
        [pltpu.SemaphoreType.DMA((3,))],
        in_specs=[pl.BlockSpec(memory_space=pltpu.HBM)] * 3,
    )
    col_a, col_b = swap_with(col_a, COLS, 0), swap_with(col_b, COLS, 1)
    row_a, row_b = swap_with(row_a, ROWS, 0), swap_with(row_b, ROWS, 1)

    cor_a, cor_b = call(corner_kernel, (col_a, col_b), ((STEPS - 1, SIZE, LANES),) * 2, [])
    cor_a, cor_b = swap_with(cor_a, ROWS, 0), swap_with(cor_b, ROWS, 1)
    edges = (col_a, col_b, row_a, row_b, cor_a, cor_b)
    tracer, sums = call(
        steps_kernel,
        (*blocks, *edges),
        (tracer.shape, (lax.axis_size("x"), 2 * SIZE, LANES)),
        [pltpu.VMEM(WORK, F32)] * 4,
    )
    count = SIZE * size_of(COLS)
    sums = lax.all_to_all(sums, "x", 0, 0, tiled=True)
    sums = call(sum_kernel, (sums,), ((lax.axis_size("y"), 2 * SIZE, LANES),), [])[0]
    sums = jnp.sum(lax.all_to_all(sums, "y", 0, 0, tiled=True), axis=0)
    totals, squares = sums[:SIZE, None], sums[SIZE:, None]
    line_mean = GUESS + totals / count
    centred = tracer - line_mean
    line_variance = squares / count - totals / count * (totals / count)
    scaled_field = centred * lax.rsqrt(line_variance + 0.0001)
    return (scaled_field, tracer)


def solution(mesh):
    mesh = Mesh(mesh.devices.reshape(2, 8, 8, 4), ("site", "rows", "y", "x"))
    placed = P(("site", "rows"), COLS, None)
    return jax.shard_map(
        shards, mesh=mesh, in_specs=(placed,) * 3, out_specs=(placed,) * 2, check_vma=False
    )
```

```python
import functools

import jax
import jax.numpy as jnp
from jax import lax
from jax.experimental import pallas as pl
from jax.experimental.pallas import tpu as pltpu
from jax.sharding import Mesh, PartitionSpec as P

STEPS = 6
SIZE = 32
LANES = 128
ROWS = "rows"
COLS = ("y", "x")
HALO = STEPS
TALL = SIZE + 2 * HALO
WIDE = SIZE + 16
BLOCK = slice(HALO, HALO + SIZE)
CENTRE = slice(8, 8 + SIZE)
WORK = (TALL, WIDE, LANES)
GUESS = 1.0
OUTER = WIDE // 8 - 1
F32 = jnp.float32
VMEM = pl.BlockSpec(memory_space=pltpu.VMEM)


def size_of(axis):
    sizes = [lax.axis_size(a) for a in ((axis,) if isinstance(axis, str) else axis)]
    return functools.reduce(lambda a, b: a * b, sizes)


def swap_with(block, axis, odd):
    pairs = []
    for low in range(odd, size_of(axis) - 1, 2):
        pairs += [(low, low + 1), (low + 1, low)]
    return lax.ppermute(block, axis, pairs)


def turned(tiles, shift):
    return pltpu.roll(tiles, shift % 8, axis=tiles.ndim - 2)


def pack_kernel(t_in, fy_in, fx_in, t, fy, fx, col_a, col_b, row_a, row_b, sems):
    blocks = ((t_in, t), (fy_in, fy), (fx_in, fx))
    copies = [pltpu.make_async_copy(src, dst, sems.at[k]) for k, (src, dst) in enumerate(blocks)]
    for copy in copies:
        copy.start()
    even_row = lax.axis_index(ROWS) % 2 == 0
    even_col = lax.axis_index(COLS) % 2 == 0
    sub = lax.broadcasted_iota(jnp.int32, (SIZE, 8, LANES), 1)
    for copy in copies:
        copy.wait()
    t_low, fy_low, fx_low = [v[:, 0:8] for v in (t, fy, fx)]
    t_high, fy_high, fx_high = [v[:, SIZE - 8 :] for v in (t, fy, fx)]
    first = (
        jnp.where(sub < 6, t_low, turned(fx_low, 6)),
        jnp.where(sub < 5, fy_low, turned(fx_low, 3)),
    )
    last = (
        jnp.where(sub >= 2, t_high, turned(fx_high, 5)),
        jnp.where(sub >= 3, fy_high, turned(fx_high, 3)),
    )
    for k in range(2):
        col_a[:, 8 * k : 8 * k + 8] = jnp.where(even_col, last[k], first[k])
        col_b[:, 8 * k : 8 * k + 8] = jnp.where(even_col, first[k], last[k])
    for out, top in ((row_a, even_row), (row_b, jnp.logical_not(even_row))):
        out[0:6] = t[pl.ds(jnp.where(top, SIZE - 6, 0), 6)]
        out[6:11] = fy[pl.ds(jnp.where(top, SIZE - 5, 0), 5)]
        out[11:16] = fx[pl.ds(jnp.where(top, SIZE - 5, 0), 5)]


def corner_kernel(col_a, col_b, cor_a, cor_b):
    even_row = lax.axis_index(ROWS) % 2 == 0
    for out, top in ((cor_a, even_row), (cor_b, jnp.logical_not(even_row))):
        at = pl.ds(jnp.where(top, SIZE - STEPS + 1, 0), STEPS - 1)
        out[:, 0:16] = col_a[at]
        out[:, 16:32] = col_b[at]


def sum_kernel(parts, out):
    total = jnp.sum(parts[...], axis=0)
    for k in range(out.shape[0]):
        out[k] = total


def scale_kernel(tracer, parts, scaled_out, end_out, scaled, mean, rate, sems):
    whole = pltpu.make_async_copy(tracer, end_out, sems.at[0])
    whole.start()
    sums = jnp.sum(parts[...], axis=0)
    count = SIZE * size_of(COLS)
    off = sums[:SIZE] / count
    mean[...] = GUESS + off
    rate[...] = lax.rsqrt(sums[SIZE:] / count - off * off + 0.0001)
    copies = [whole]
    for k in range(4):
        some = pl.ds(k * (SIZE // 4), SIZE // 4)
        for y in range(k * (SIZE // 4), (k + 1) * (SIZE // 4)):
            scaled[y] = (tracer[y] - mean[pl.ds(y, 1)]) * rate[pl.ds(y, 1)]
        copies.append(pltpu.make_async_copy(scaled.at[some], scaled_out.at[some], sems.at[1 + k]))
        copies[-1].start()
    for copy in copies:
        copy.wait()


def beside(packed, west):
    one, two = packed[:, 0:8], packed[:, 8:16]
    sub = lax.broadcasted_iota(jnp.int32, one.shape, 1)
    if west:
        return one, two, jnp.where(sub < 5, turned(one, 3), turned(two, 5))
    return one, two, jnp.where(sub < 2, turned(one, 2), turned(two, 5))


def moved_on(mid, below, above, left, right, flow_y, flow_x):
    spread = (below + above) + (left + right)
    return 0.8 * mid + 0.05 * spread - flow_y * (above - below) - flow_x * (right - left)


def sides():
    row, col = lax.axis_index(ROWS), lax.axis_index(COLS)
    return row == 0, row == lax.axis_size(ROWS) - 1, col > 0, col < size_of(COLS) - 1


def at(j):
    return pl.ds(8 * j, 8)


def sublanes():
    sub = lax.broadcasted_iota(jnp.int32, (8, LANES), 0)
    return sub == 0, sub == 7


def steps_kernel(t, fy, fx, col_a, col_b, row_a, row_b, p0, p1, p2, p3, p4, p5, cy, cx, end, sums, total, square):
    even_row, even_col = lax.axis_index(ROWS) % 2 == 0, lax.axis_index(COLS) % 2 == 0
    first_row, last_row, has_west, has_east = sides()
    for src, dst in ((t, p0), (fy, cy), (fx, cx)):
        dst[BLOCK, CENTRE] = src[...]
    west, east = jnp.where(even_col, col_b[...], col_a[...]), jnp.where(even_col, col_a[...], col_b[...])
    for v, j, is_west in ((west, 0, True), (east, OUTER, False)):
        for tile, dst in zip(beside(v, is_west), (p0, cy, cx)):
            dst[BLOCK, at(j)] = tile
    south, north = jnp.where(even_row, row_b[...], row_a[...]), jnp.where(even_row, row_a[...], row_b[...])
    for (b, e), dst in zip(((0, 6), (6, 11), (11, 16)), (p0, cy, cx)):
        dst[HALO - (e - b) : HALO, CENTRE] = south[b:e]
        dst[HALO + SIZE : HALO + SIZE + e - b, CENTRE] = north[b:e]
    lowest, highest = sublanes()

    def stepped(src, y, tiles):
        around = [j for j in range(tiles[0] - 1, tiles[-1] + 2) if 0 <= j <= OUTER]
        mid = {j: src[y, at(j)] for j in around}
        up = {j: turned(v, 1) for j, v in mid.items()}
        down = {j: turned(v, -1) for j, v in mid.items()}
        out = []
        for j in tiles:
            left = jnp.where(lowest, up[j - 1], up[j]) if j > 0 else up[j]
            right = jnp.where(highest, down[j + 1], down[j]) if j < OUTER else down[j]
            new = moved_on(mid[j], src[y - 1, at(j)], src[y + 1, at(j)], left, right, cy[y, at(j)], cx[y, at(j)])
            if j == 0:
                new = jnp.where(has_west, new, 0.0)
            if j == OUTER:
                new = jnp.where(has_east, new, 0.0)
            out.append(new)
        return out

    fields = (p0, p1, p2, p3, p4, p5)
    middle, everything = list(range(1, OUTER)), list(range(OUTER + 1))
    for step, (src, dst) in enumerate(zip(fields, fields[1:]), start=1):
        for y in list(range(step, HALO)) + list(range(HALO + SIZE, TALL - step)):
            outside = first_row if y < HALO else last_row
            for j, new in zip(middle, stepped(src, y, middle)):
                dst[y, at(j)] = jnp.where(outside, 0.0, new)

        def body(i, _, src=src, dst=dst):
            for y in (2 * i + HALO, 2 * i + HALO + 1):
                for j, new in zip(everything, stepped(src, y, everything)):
                    dst[y, at(j)] = new
            return 0

        lax.fori_loop(0, SIZE // 2, body, 0)

    def final(i, _):
        for y in (2 * i, 2 * i + 1):
            new = stepped(p5, y + HALO, middle)
            for j, v in zip(middle, new):
                end[y, at(j - 1)] = v
            total[y], square[y] = moments(new)
        return 0

    lax.fori_loop(0, SIZE // 2, final, 0)
    sums[0:SIZE] = jnp.sum(total[...], axis=1)
    sums[SIZE : 2 * SIZE] = jnp.sum(square[...], axis=1)


def moments(tiles):
    moved = [v - GUESS for v in tiles]
    squares = [v * v for v in moved]
    add = lambda v: functools.reduce(lambda a, b: a + b, v)
    return add(moved), add(squares)


def patch_kernel(p0, p1, p2, p3, p4, p5, cy, cx, cor_a, cor_b, end, sums, end_out, sums_out, total, square):
    even_row, even_col = lax.axis_index(ROWS) % 2 == 0, lax.axis_index(COLS) % 2 == 0
    first_row, last_row, has_west, has_east = sides()
    lowest, highest = sublanes()
    fields = (p0, p1, p2, p3, p4, p5)
    end_out[...] = end[...]
    for k in range(sums_out.shape[0]):
        sums_out[k] = sums[...]
    south, north = jnp.where(even_row, cor_b[...], cor_a[...]), jnp.where(even_row, cor_a[...], cor_b[...])
    for is_south, corner, outside in ((True, south, first_row), (False, north, last_row)):
        row = (lambda r: r) if is_south else (lambda r: TALL - 1 - r)
        inner_tiles = {}
        for is_west, inside in ((True, has_west), (False, has_east)):
            packed = jnp.where(even_col == is_west, corner[:, 16:32], corner[:, 0:16])
            order = list(range(HALO - 1)) if is_south else list(range(HALO - 1))[::-1]
            tracer, flow_y, flow_x = [
                {r: tile[i] for r, i in enumerate(order, start=1)} for tile in beside(packed, is_west)
            ]
            j0, j1, j2 = (0, 1, 2) if is_west else (OUTER, OUTER - 1, OUTER - 2)
            tracer[0] = jnp.zeros((8, LANES), F32)
            fixed = {(r, j0): v for r, v in tracer.items()}
            for step in range(1, STEPS + 1):
                field = fields[step - 1]
                get = lambda r, j: fixed[r, j] if (r, j) in fixed else field[row(r), at(j)]
                now = {}
                for r in range(step, HALO + step):
                    for j in (j0, j1) if step < STEPS else (j1,):
                        mid = get(r, j)
                        near, far = (get(r, j2 if j == j1 else j1), get(r, j0) if j == j1 else mid)
                        lower, higher = (far, near) if is_west else (near, far)
                        left = jnp.where(lowest, turned(lower, 1), turned(mid, 1)) if lower is not mid else turned(mid, 1)
                        right = jnp.where(highest, turned(higher, -1), turned(mid, -1)) if higher is not mid else turned(mid, -1)
                        below, above = (get(r - 1, j), get(r + 1, j)) if is_south else (get(r + 1, j), get(r - 1, j))
                        of_corner = j == j0 and r < HALO
                        flows = (flow_y[r], flow_x[r]) if of_corner else (cy[row(r), at(j)], cx[row(r), at(j)])
                        new = moved_on(mid, below, above, left, right, *flows)
                        if j == j0:
                            new = jnp.where(inside, new, 0.0)
                        if r < HALO:
                            new = jnp.where(outside, 0.0, new)
                        now[r, j] = new
                fixed = now
            for r in range(HALO, 2 * HALO):
                inner_tiles[r, j1] = fixed[r, j1]
        for r in range(HALO, 2 * HALO):
            y = row(r) - HALO
            new = [inner_tiles[r, j] if (r, j) in inner_tiles else end[y, at(j - 1)] for j in range(1, OUTER)]
            for j in (1, OUTER - 1):
                end_out[y, at(j - 1)] = new[j - 1]
            i = y if is_south else y - SIZE + 2 * HALO
            total[i], square[i] = moments(new)
    total, square = jnp.sum(total[...], axis=1), jnp.sum(square[...], axis=1)
    for k in range(sums_out.shape[0]):
        for b, v in ((0, total), (SIZE, square)):
            sums_out[k, b : b + HALO] = v[:HALO]
            sums_out[k, b + SIZE - HALO : b + SIZE] = v[HALO:]


def call(kernel, args, outs, scratch, in_specs=None):
    specs = in_specs or [VMEM] * len(args)
    return pl.pallas_call(
        kernel,
        out_shape=[pltpu.VMEM(shape, F32) for shape in outs],
        in_specs=specs,
        out_specs=[VMEM] * len(outs),
        scratch_shapes=scratch,
        compiler_params=pltpu.CompilerParams(vmem_limit_bytes=16 * 2**20),
    )(*[pltpu.with_memory_space_constraint(a, s.memory_space) for a, s in zip(args, specs)])


def shards(tracer, flow_y, flow_x):
    columns, rows = (SIZE, 16, LANES), (16, SIZE, LANES)
    *blocks, col_a, col_b, row_a, row_b = call(
        pack_kernel,
        (tracer, flow_y, flow_x),
        (tracer.shape,) * 3 + (columns,) * 2 + (rows,) * 2,
        [pltpu.SemaphoreType.DMA((3,))],
        in_specs=[pl.BlockSpec(memory_space=pltpu.HBM)] * 3,
    )
    col_a, col_b = swap_with(col_a, COLS, 0), swap_with(col_b, COLS, 1)
    row_a, row_b = swap_with(row_a, ROWS, 0), swap_with(row_b, ROWS, 1)

    cor_a, cor_b = call(corner_kernel, (col_a, col_b), ((STEPS - 1, SIZE, LANES),) * 2, [])
    cor_a, cor_b = swap_with(cor_a, ROWS, 0), swap_with(cor_b, ROWS, 1)
    partial = pltpu.VMEM((SIZE, 8, LANES), F32)
    *fields, tracer, sums = call(
        steps_kernel,
        (*blocks, col_a, col_b, row_a, row_b),
        (WORK,) * (STEPS + 2) + (tracer.shape, (2 * SIZE, LANES)),
        [partial] * 2,
    )
    partial = pltpu.VMEM((2 * HALO, 8, LANES), F32)
    tracer, sums = call(
        patch_kernel,
        (*fields, cor_a, cor_b, tracer, sums),
        (tracer.shape, (lax.axis_size("x"), 2 * SIZE, LANES)),
        [partial] * 2,
    )
    sums = lax.all_to_all(sums, "x", 0, 0, tiled=True)
    sums = call(sum_kernel, (sums,), ((lax.axis_size("y"), 2 * SIZE, LANES),), [])[0]
    sums = lax.all_to_all(sums, "y", 0, 0, tiled=True)
    outer = pl.BlockSpec(memory_space=pltpu.HBM)
    return tuple(
        pl.pallas_call(
            scale_kernel,
            out_shape=[jax.ShapeDtypeStruct(tracer.shape, F32)] * 2,
            in_specs=[VMEM] * 2,
            out_specs=[outer] * 2,
            scratch_shapes=[
                pltpu.VMEM(tracer.shape, F32),
                pltpu.VMEM((SIZE, LANES), F32),
                pltpu.VMEM((SIZE, LANES), F32),
                pltpu.SemaphoreType.DMA((5,)),
            ],
            compiler_params=pltpu.CompilerParams(vmem_limit_bytes=16 * 2**20),
        )(*[pltpu.with_memory_space_constraint(v, pltpu.VMEM) for v in (tracer, sums)])
    )


def solution(mesh):
    mesh = Mesh(mesh.devices.reshape(2, 8, 8, 4), ("site", "rows", "y", "x"))
    placed = P(("site", "rows"), COLS, None)
    return jax.shard_map(
        shards, mesh=mesh, in_specs=(placed,) * 3, out_specs=(placed,) * 2, check_vma=False
    )
```

```python
import functools

import jax
import jax.numpy as jnp
from jax import lax
from jax.experimental import pallas as pl
from jax.experimental.pallas import tpu as pltpu
from jax.sharding import Mesh, PartitionSpec as P

STEPS = 6
SIZE = 32
LANES = 128
ROWS = "rows"
COLS = ("y", "x")
HALO = STEPS
TALL = SIZE + 2 * HALO
WIDE = SIZE + 16
BLOCK = slice(HALO, HALO + SIZE)
CENTRE = slice(8, 8 + SIZE)
WORK = (TALL, WIDE, LANES)
GUESS = 1.0
TOGETHER = 16
OUTER = WIDE // 8 - 1
F32 = jnp.float32
VMEM = pl.BlockSpec(memory_space=pltpu.VMEM)


def size_of(axis):
    sizes = [lax.axis_size(a) for a in ((axis,) if isinstance(axis, str) else axis)]
    return functools.reduce(lambda a, b: a * b, sizes)


SWAP = {ROWS: False, COLS: True}
WAVE = (
    ((ROWS, 1), (COLS, 1)),
    ((ROWS, 0), (COLS, 0)),
    ((COLS, 1), (ROWS, 1)),
    ((COLS, 0), (ROWS, 0)),
    ((COLS, 1), (ROWS, 1)),
    ((COLS, 0), (ROWS, 0)),
)


def pairs_along(axis, k):
    count = size_of(axis)
    if SWAP[axis]:
        return [p for low in range(k, count - 1, 2) for p in ((low, low + 1), (low + 1, low))]
    return [(low + k, low + 1 - k) for low in range(count - 1)]


def sent(block, wave):
    rows, cols, pairs = size_of(ROWS), size_of(COLS), []
    for site, (axis, k) in enumerate(WAVE[wave][: lax.axis_size("site")]):
        for one, two in pairs_along(axis, k):
            for other in range(cols if axis == ROWS else rows):
                at_one, at_two = ((one, other), (two, other)) if axis == ROWS else ((other, one), (other, two))
                pairs.append(tuple((site * rows + r) * cols + c for r, c in (at_one, at_two)))
    return lax.ppermute(block, ("site", ROWS, *COLS), pairs)


def columns_first():
    return lax.axis_index("site") == 1


def even(axis):
    return lax.axis_index(axis) % 2 == 0


def to_send(axis, high, low):
    if not SWAP[axis]:
        return high, low
    return jnp.where(even(axis), high, low), jnp.where(even(axis), low, high)


def received(axis, one, two):
    if not SWAP[axis]:
        return one, two
    return jnp.where(even(axis), two, one), jnp.where(even(axis), one, two)


def starts(axis, high, low):
    if not SWAP[axis]:
        return high, low
    return jnp.where(even(axis), high, low), jnp.where(even(axis), low, high)


def turned(tiles, shift):
    return pltpu.roll(tiles, shift % 8, axis=tiles.ndim - 2)


def pack_kernel(t_in, fy_in, fx_in, t, fy, fx, one, two, three, four, sems):
    blocks = ((t_in, t), (fy_in, fy), (fx_in, fx))
    copies = [pltpu.make_async_copy(src, dst, sems.at[k]) for k, (src, dst) in enumerate(blocks)]
    for copy in copies:
        copy.start()
    for copy in copies:
        copy.wait()
    low, high = [packed([v[:, cut] for v in (t, fy, fx)], is_low) for cut, is_low in ((slice(0, 8), True), (slice(SIZE - 8, SIZE), False))]
    cols = [jnp.concatenate(v, axis=1) for v in zip(*[to_send(COLS, high[k], low[k]) for k in range(2)])]
    rows = []
    for k in range(2):
        parts = [src[pl.ds(starts(ROWS, SIZE - w, 0)[k], w)] for src, w in ((t, 6), (fy, 5), (fx, 5))]
        rows.append(jnp.concatenate(parts, axis=0).reshape(SIZE, 16, LANES))
    for k, (early, late) in ((1, (one, three)), (0, (two, four))):
        early[...] = jnp.where(columns_first(), cols[k], rows[k])
        late[...] = jnp.where(columns_first(), rows[k], cols[k])


def packed(tiles, is_low):
    t, fy, fx = tiles
    sub = lax.broadcasted_iota(jnp.int32, t.shape, 1)
    if is_low:
        return jnp.where(sub < 6, t, turned(fx, 6)), jnp.where(sub < 5, fy, turned(fx, 3))
    return jnp.where(sub >= 2, t, turned(fx, 5)), jnp.where(sub >= 3, fy, turned(fx, 3))


def corner_kernel(one, two, cor_b, cor_a):
    depth = STEPS - 1
    along_rows = []
    for cut in starts(ROWS, SIZE - depth, 0):
        pieces = received(COLS, two[pl.ds(cut, depth)], one[pl.ds(cut, depth)])
        along_rows.append(jnp.concatenate(pieces, axis=1).reshape(2 * depth, 16, LANES))
    along_cols = [[], []]
    as_rows = [v[...].reshape(16, SIZE, LANES) for v in (two, one)]
    for v, first in zip(received(ROWS, *as_rows), ((1, 6, 11), (0, 6, 11))):
        low, high = [
            packed([v[b : b + depth, cut] for b in first], is_low)
            for cut, is_low in ((slice(0, 8), True), (slice(SIZE - 8, SIZE), False))
        ]
        for out, tiles in zip(along_cols, zip(*[to_send(COLS, high[j], low[j]) for j in range(2)])):
            out.append(jnp.concatenate(tiles, axis=1))
    for out, rows, cols in zip((cor_a, cor_b), along_rows, along_cols):
        out[...] = jnp.where(columns_first(), rows, jnp.concatenate(cols, axis=0))


def sum_kernel(parts, out):
    total = jnp.sum(parts[...], axis=0)
    for k in range(out.shape[0]):
        out[k] = total


def scale_kernel(tracer, parts, scaled_out, end_out, scaled, mean, rate, sems):
    whole = pltpu.make_async_copy(tracer, end_out, sems.at[0])
    whole.start()
    sums = jnp.sum(parts[...], axis=0)
    count = SIZE * size_of(COLS)
    off = sums[:SIZE] / count
    mean[...] = GUESS + off
    rate[...] = lax.rsqrt(sums[SIZE:] / count - off * off + 0.0001)
    copies = [whole]
    for k in range(4):
        some = pl.ds(k * (SIZE // 4), SIZE // 4)
        for y in range(k * (SIZE // 4), (k + 1) * (SIZE // 4)):
            scaled[y] = (tracer[y] - mean[pl.ds(y, 1)]) * rate[pl.ds(y, 1)]
        copies.append(pltpu.make_async_copy(scaled.at[some], scaled_out.at[some], sems.at[1 + k]))
        copies[-1].start()
    for copy in copies:
        copy.wait()


def beside(packed, west):
    one, two = packed[:, 0:8], packed[:, 8:16]
    sub = lax.broadcasted_iota(jnp.int32, one.shape, 1)
    if west:
        return one, two, jnp.where(sub < 5, turned(one, 3), turned(two, 5))
    return one, two, jnp.where(sub < 2, turned(one, 2), turned(two, 5))


def moved_on(mid, below, above, left, right, flow_y, flow_x):
    spread = (below + above) + (left + right)
    return 0.8 * mid + 0.05 * spread - flow_y * (above - below) - flow_x * (right - left)


def sides():
    row, col = lax.axis_index(ROWS), lax.axis_index(COLS)
    return row == 0, row == lax.axis_size(ROWS) - 1, col > 0, col < size_of(COLS) - 1


def at(j):
    return pl.ds(8 * j, 8)


def sublanes():
    sub = lax.broadcasted_iota(jnp.int32, (8, LANES), 0)
    return sub == 0, sub == 7


def steps_kernel(t, fy, fx, one, two, three, four, p0, p1, p2, p3, p4, p5, cy, cx, end, sums, total, square):
    first_row, last_row, has_west, has_east = sides()
    for src, dst in ((t, p0), (fy, cy), (fx, cx)):
        dst[BLOCK, CENTRE] = src[...]
    first = columns_first()
    col_a, col_b = jnp.where(first, two[...], four[...]), jnp.where(first, one[...], three[...])
    row_a, row_b = jnp.where(first, four[...], two[...]), jnp.where(first, three[...], one[...])
    west, east = received(COLS, col_a, col_b)
    for v, j, is_west in ((west, 0, True), (east, OUTER, False)):
        for tile, dst in zip(beside(v, is_west), (p0, cy, cx)):
            dst[BLOCK, at(j)] = tile
    south, north = received(ROWS, *[v.reshape(16, SIZE, LANES) for v in (row_a, row_b)])
    for (b, e), dst in zip(((0, 6), (6, 11), (11, 16)), (p0, cy, cx)):
        dst[HALO - (e - b) : HALO, CENTRE] = south[b:e]
        dst[HALO + SIZE : HALO + SIZE + e - b, CENTRE] = north[b:e]
    lowest, highest = sublanes()

    def stepped(src, first, count, tiles):
        around = [j for j in range(tiles[0] - 1, tiles[-1] + 2) if 0 <= j <= OUTER]
        rows = [{j: src[first + k, at(j)] for j in (around if 0 <= k < count else tiles)} for k in range(-1, count + 1)]
        for k in range(count):
            y, (below, mid, above) = first + k, rows[k : k + 3]
            up = {j: turned(v, 1) for j, v in mid.items()}
            down = {j: turned(v, -1) for j, v in mid.items()}
            out = []
            for j in tiles:
                left = jnp.where(lowest, up[j - 1], up[j]) if j > 0 else up[j]
                right = jnp.where(highest, down[j + 1], down[j]) if j < OUTER else down[j]
                new = moved_on(mid[j], below[j], above[j], left, right, cy[y, at(j)], cx[y, at(j)])
                if j == 0:
                    new = jnp.where(has_west, new, 0.0)
                if j == OUTER:
                    new = jnp.where(has_east, new, 0.0)
                out.append(new)
            yield y, out

    fields = (p0, p1, p2, p3, p4, p5)
    middle, everything = list(range(1, OUTER)), list(range(OUTER + 1))
    for step, (src, dst) in enumerate(zip(fields, fields[1:]), start=1):
        for first, outside in ((step, first_row), (HALO + SIZE, last_row)):
            for y, new in stepped(src, first, HALO - step, middle):
                for j, v in zip(middle, new):
                    dst[y, at(j)] = jnp.where(outside, 0.0, v)

        def body(i, _, src=src, dst=dst):
            for y, new in stepped(src, TOGETHER * i + HALO, TOGETHER, everything):
                for j, v in zip(everything, new):
                    dst[y, at(j)] = v
            return 0

        lax.fori_loop(0, SIZE // TOGETHER, body, 0)

    def final(i, _):
        for y, new in stepped(p5, TOGETHER * i + HALO, TOGETHER, middle):
            for j, v in zip(middle, new):
                end[y - HALO, at(j - 1)] = v
            total[y - HALO], square[y - HALO] = moments(new)
        return 0

    lax.fori_loop(0, SIZE // TOGETHER, final, 0)
    sums[0:SIZE] = jnp.sum(total[...], axis=1)
    sums[SIZE : 2 * SIZE] = jnp.sum(square[...], axis=1)


def moments(tiles):
    moved = [v - GUESS for v in tiles]
    squares = [v * v for v in moved]
    add = lambda v: functools.reduce(lambda a, b: a + b, v)
    return add(moved), add(squares)


def patch_kernel(p0, p1, p2, p3, p4, p5, cy, cx, cor_a, cor_b, end, sums, end_out, sums_out, total, square):
    first_row, last_row, has_west, has_east = sides()
    lowest, highest = sublanes()
    fields = (p0, p1, p2, p3, p4, p5)
    end_out[...] = end[...]
    for k in range(sums_out.shape[0]):
        sums_out[k] = sums[...]
    depth = STEPS - 1
    lower, upper = received(ROWS, *[v[...].reshape(depth, SIZE, LANES) for v in (cor_a, cor_b)])
    west, east = received(COLS, cor_a[...], cor_b[...])
    corners = [
        [jnp.where(columns_first(), v[:, 16 * k : 16 * k + 16], u[b : b + depth]) for k, u in enumerate((west, east))]
        for v, b in ((lower, 0), (upper, depth))
    ]
    for is_south, corner, outside in ((True, corners[0], first_row), (False, corners[1], last_row)):
        row = (lambda r: r) if is_south else (lambda r: TALL - 1 - r)
        inner_tiles = {}
        for is_west, inside, of_corner in ((True, has_west, corner[0]), (False, has_east, corner[1])):
            order = list(range(HALO - 1)) if is_south else list(range(HALO - 1))[::-1]
            tracer, flow_y, flow_x = [
                {r: tile[i] for r, i in enumerate(order, start=1)} for tile in beside(of_corner, is_west)
            ]
            j0, j1, j2 = (0, 1, 2) if is_west else (OUTER, OUTER - 1, OUTER - 2)
            tracer[0] = jnp.zeros((8, LANES), F32)
            fixed = {(r, j0): v for r, v in tracer.items()}
            for step in range(1, STEPS + 1):
                field = fields[step - 1]
                get = lambda r, j: fixed[r, j] if (r, j) in fixed else field[row(r), at(j)]
                now = {}
                for r in range(step, HALO + step):
                    for j in (j0, j1) if step < STEPS else (j1,):
                        mid = get(r, j)
                        near, far = (get(r, j2 if j == j1 else j1), get(r, j0) if j == j1 else mid)
                        lower, higher = (far, near) if is_west else (near, far)
                        left = jnp.where(lowest, turned(lower, 1), turned(mid, 1)) if lower is not mid else turned(mid, 1)
                        right = jnp.where(highest, turned(higher, -1), turned(mid, -1)) if higher is not mid else turned(mid, -1)
                        below, above = (get(r - 1, j), get(r + 1, j)) if is_south else (get(r + 1, j), get(r - 1, j))
                        flows = (flow_y[r], flow_x[r]) if j == j0 and r < HALO else (cy[row(r), at(j)], cx[row(r), at(j)])
                        new = moved_on(mid, below, above, left, right, *flows)
                        if j == j0:
                            new = jnp.where(inside, new, 0.0)
                        if r < HALO:
                            new = jnp.where(outside, 0.0, new)
                        now[r, j] = new
                fixed = now
            for r in range(HALO, 2 * HALO):
                inner_tiles[r, j1] = fixed[r, j1]
        for r in range(HALO, 2 * HALO):
            y = row(r) - HALO
            new = [inner_tiles[r, j] if (r, j) in inner_tiles else end[y, at(j - 1)] for j in range(1, OUTER)]
            for j in (1, OUTER - 1):
                end_out[y, at(j - 1)] = new[j - 1]
            i = y if is_south else y - SIZE + 2 * HALO
            total[i], square[i] = moments(new)
    total, square = jnp.sum(total[...], axis=1), jnp.sum(square[...], axis=1)
    for k in range(sums_out.shape[0]):
        for b, v in ((0, total), (SIZE, square)):
            sums_out[k, b : b + HALO] = v[:HALO]
            sums_out[k, b + SIZE - HALO : b + SIZE] = v[HALO:]


def call(kernel, args, outs, scratch, in_specs=None):
    specs = in_specs or [VMEM] * len(args)
    return pl.pallas_call(
        kernel,
        out_shape=[pltpu.VMEM(shape, F32) for shape in outs],
        in_specs=specs,
        out_specs=[VMEM] * len(outs),
        scratch_shapes=scratch,
        compiler_params=pltpu.CompilerParams(vmem_limit_bytes=16 * 2**20),
    )(*[pltpu.with_memory_space_constraint(a, s.memory_space) for a, s in zip(args, specs)])


def shards(tracer, flow_y, flow_x):
    *blocks, one, two, three, four = call(
        pack_kernel,
        (tracer, flow_y, flow_x),
        (tracer.shape,) * 3 + ((SIZE, 16, LANES),) * 4,
        [pltpu.SemaphoreType.DMA((3,))],
        in_specs=[pl.BlockSpec(memory_space=pltpu.HBM)] * 3,
    )
    one, two, three, four = [sent(v, k) for k, v in enumerate((one, two, three, four))]
    cor_b, cor_a = call(corner_kernel, (one, two), ((2 * STEPS - 2, 16, LANES),) * 2, [])
    cor_b, cor_a = sent(cor_b, 4), sent(cor_a, 5)
    partial = pltpu.VMEM((SIZE, 8, LANES), F32)
    *fields, tracer, sums = call(
        steps_kernel,
        (*blocks, one, two, three, four),
        (WORK,) * (STEPS + 2) + (tracer.shape, (2 * SIZE, LANES)),
        [partial] * 2,
    )
    partial = pltpu.VMEM((2 * HALO, 8, LANES), F32)
    tracer, sums = call(
        patch_kernel,
        (*fields, cor_a, cor_b, tracer, sums),
        (tracer.shape, (lax.axis_size("x"), 2 * SIZE, LANES)),
        [partial] * 2,
    )
    sums = lax.all_to_all(sums, "x", 0, 0, tiled=True)
    sums = call(sum_kernel, (sums,), ((lax.axis_size("y"), 2 * SIZE, LANES),), [])[0]
    sums = lax.all_to_all(sums, "y", 0, 0, tiled=True)
    outer = pl.BlockSpec(memory_space=pltpu.HBM)
    return tuple(
        pl.pallas_call(
            scale_kernel,
            out_shape=[jax.ShapeDtypeStruct(tracer.shape, F32)] * 2,
            in_specs=[VMEM] * 2,
            out_specs=[outer] * 2,
            scratch_shapes=[
                pltpu.VMEM(tracer.shape, F32),
                pltpu.VMEM((SIZE, LANES), F32),
                pltpu.VMEM((SIZE, LANES), F32),
                pltpu.SemaphoreType.DMA((5,)),
            ],
            compiler_params=pltpu.CompilerParams(vmem_limit_bytes=16 * 2**20),
        )(*[pltpu.with_memory_space_constraint(v, pltpu.VMEM) for v in (tracer, sums)])
    )


def solution(mesh):
    mesh = Mesh(mesh.devices.reshape(2, 8, 8, 4), ("site", "rows", "y", "x"))
    placed = P(("site", "rows"), COLS, None)
    return jax.shard_map(
        shards, mesh=mesh, in_specs=(placed,) * 3, out_specs=(placed,) * 2, check_vma=False
    )
```
